32 devices in a mesh: grp: 2 (over y), tok: 8 (over z, x), head: 2 (over core).
Axes of the slice: x: 2, y: 2, z: 4, core: 2. Of those that a mesh axis runs over, the one named last changes fastest.
Arguments:
- events: bfloat16 [16384, 1024], P(('grp', 'tok')), parts along dimension 0, may hold values from -6 to 6
- uvqk_weight: bfloat16 [1024, 4, 1024], P(None, None, 'head'), may hold values from -0.1875 to 0.1875
- out_weight: bfloat16 [1024, 1024], P('head'), may hold values from -0.1875 to 0.1875
- segments: int32 [16, 1024], P(('grp', 'tok')), parts along dimension 0, may hold values from 0 to 7, never falling along the last dimension, each value on 1 to 512 neighbouring positions
Outputs:
- targets: bfloat16 [16384, 1024], P(('grp', 'tok'), 'head'), parts along dimension 0
The draws below stay inside these ranges and needn't reach their ends.
There are 2 independent parts, one for each index of `grp`. The reference program is written for one: setup_inputs(seed, part) draws one part's arguments, and reference() takes and returns one part's arrays. A program takes and returns all parts, laid end to end along the dimension named above; an argument that names none is the same for every part. Nothing has to cross between parts.
Inputs may be any that keep to these rules, and one draw needn't show every extreme that they name: `segments`: in each row numbers never fall; every user 0 to 7 holds 1 to 512 consecutive rows of its owner, and some user holds exactly 512.
All inputs are finite; a program needn't handle non-finite values.
Results may differ from the reference program's by a relative error of at most 0.007.
Values may be sent and summed in bfloat16 or wider, within the bound.
No kernel may reach another device: no remote copies, remote signals or barrier semaphores. Data moves between devices by JAX's collectives and lax.ppermute only.
A program may use at most 64 MiB of HBM per device.

```python
import math
import jax
import jax.numpy as jnp
import numpy as np
from jax import lax

D = 1024
HD = 128
TOK_DEV = 1024
USERS_OWN = 8
BLK = 128
MAXLEN = 512
SLOT = 128
TOKENS = 8192
HGRP = 2
N_TOK = 8


def block_levels(stream_key, dims, split, low, top_value):
    loudness = 1.0
    for dim, blocks in split:
        heights = jax.random.uniform(jax.random.fold_in(jax.random.fold_in(stream_key, 6), dim), (blocks,), jnp.float32, low / len(split), top_value / len(split))
        loudness = loudness * jnp.repeat(jnp.exp(heights), dims[dim] // blocks).reshape((-1,) + (1,) * (len(dims) - 1 - dim))
    return loudness


def profile(number_of, total, limit, lean):
    loads = [(1 << 20) // math.isqrt(rank ** lean) + 1 for rank in range(2, number_of + 1)]
    rest, holding = total - limit - (number_of - 1), [1] * (number_of - 1)
    while rest > 0:
        candidates = [i for i in range(number_of - 1) if holding[i] < limit]
        pool, remaining = sum([loads[i] for i in candidates]), rest
        for i in candidates:
            extra = min(limit - holding[i], max(1, remaining * loads[i] // pool), rest)
            holding[i] = holding[i] + extra
            rest = rest - extra
    return np.array([limit] + holding)


def ragged(key, amount, total, most, lean):
    if amount == 2:
        one = jax.random.randint(key, (), max(1, total - most), min(most, total - 1) + 1)
        return jnp.stack([one, total - one])
    sizes = jnp.asarray(profile(amount, total, most, lean), jnp.int32)
    twos = (amount - 1) // 2
    donor, receiver = sizes[1:1 + 2 * twos:2], sizes[2:2 + 2 * twos:2]
    room = jnp.minimum(donor - 1, most - receiver)
    moved = jax.random.randint(jax.random.fold_in(key, 1), (twos,), 0, 1 << 20) % (room + 1)
    sizes = sizes.at[1:1 + 2 * twos:2].set(donor - moved).at[2:2 + 2 * twos:2].set(receiver + moved)
    return sizes[jax.random.permutation(jax.random.fold_in(key, 2), amount)]


def scatter_about(rng, extent, deviation, reach, split=(), kind=jnp.bfloat16):
    array = deviation * jax.random.normal(rng, extent, jnp.float32)
    if split:
        array = array * block_levels(rng, extent, split, -0.22, 0.18)
    return jnp.clip(array, -reach, reach).astype(kind)


def setup_inputs(seed: int = 0, part: int = 0) -> dict:
    seeds = jax.random.split(jax.random.key(seed), 5)
    own_keys = jax.random.split(jax.random.fold_in(seeds[4], part), 5)
    events = scatter_about(own_keys[0], (TOKENS, D), 1.0, 6.0, ((0, 8),))
    uvqk_weight = scatter_about(seeds[1], (D, 4, D), D ** -0.5, 0.1875, ((2, 2),))
    out_weight = scatter_about(seeds[2], (D, D), D ** -0.5, 0.1875, ((0, 2),))
    segments = jax.vmap(lambda own: jnp.searchsorted(jnp.cumsum(ragged(own, USERS_OWN, TOK_DEV, MAXLEN, 2)), jnp.arange(TOK_DEV), side="right"))(jax.random.split(own_keys[3], N_TOK)).reshape((N_TOK, TOK_DEV)).astype(jnp.int32)
    return {"events": events, "uvqk_weight": uvqk_weight, "out_weight": out_weight, "segments": segments}


def project(features, uvqk_weight):
    mixed_rows = jnp.einsum('td,dkf->tkf', features.astype(jnp.float32), uvqk_weight.astype(jnp.float32))
    rounded = jax.nn.silu(mixed_rows).astype(jnp.bfloat16)
    return lax.optimization_barrier(rounded)

def positions(segments, user_count):
    user_ids = jnp.arange(user_count, dtype=jnp.int32)
    member = (segments[:, None] == user_ids[None, :]).astype(jnp.int32)
    counts = lax.optimization_barrier(jnp.sum(member, axis=0))
    firsts = jnp.cumsum(counts) - counts
    first_row = lax.optimization_barrier(jnp.sum(member * firsts[None, :], axis=1))
    return jnp.arange(segments.shape[0], dtype=jnp.int32) - first_row

def attend(uvqk_rows, segments):
    row_count = uvqk_rows.shape[0]
    heads_here = uvqk_rows.shape[2] // HD
    split_rows = uvqk_rows.reshape(row_count, 4, heads_here, HD)
    gate_rows = split_rows[:, 0]
    value_rows = split_rows[:, 1].astype(jnp.float32)
    query_rows = split_rows[:, 2]
    key_rows = split_rows[:, 3].astype(jnp.float32)
    blocks = positions(segments, USERS_OWN) // BLK
    qblock = min(512, row_count)
    block_count = row_count // qblock

    def one_block(block_index):
        begin_row = block_index * qblock
        query_part = lax.dynamic_slice_in_dim(query_rows, begin_row, qblock, 0).astype(jnp.float32)
        gate_part = lax.dynamic_slice_in_dim(gate_rows, begin_row, qblock, 0).astype(jnp.float32)
        seg_part = lax.dynamic_slice_in_dim(segments, begin_row, qblock, 0)
        blk_part = lax.dynamic_slice_in_dim(blocks, begin_row, qblock, 0)
        scores = jnp.einsum('qhe,khe->hqk', query_part, key_rows) * HD ** (-0.5)
        allowed = (seg_part[:, None] == segments[None, :]) & (blocks[None, :] <= blk_part[:, None])
        weights = jnp.where(allowed[None], jax.nn.silu(scores), 0.0).astype(jnp.bfloat16)
        weights = lax.optimization_barrier(weights).astype(jnp.float32)
        mixed_rows = jnp.einsum('hqk,khe->qhe', weights, value_rows)
        normed = mixed_rows * lax.rsqrt(lax.optimization_barrier(jnp.mean(mixed_rows * mixed_rows, axis=-1, keepdims=True)) + 1e-06)
        return (normed * gate_part).astype(jnp.bfloat16).reshape(qblock, heads_here * HD)
    outputs = lax.map(one_block, jnp.arange(block_count, dtype=jnp.int32))
    return outputs.reshape(row_count, heads_here * HD)

def reference(events, uvqk_weight, out_weight, segments):
    grid = events.reshape(N_TOK, N_TOK, SLOT, D)
    group_width = D // HGRP

    def per_owner(owner_index):
        owner_rows = lax.dynamic_index_in_dim(grid, owner_index, 1, keepdims=False).reshape(TOK_DEV, D)
        owner_segments = lax.dynamic_index_in_dim(segments, owner_index, 0, keepdims=False)
        attended = attend(project(owner_rows, uvqk_weight), owner_segments)
        branch = jnp.zeros((TOK_DEV, D), jnp.float32)
        for group in range(HGRP):
            columns = attended[:, group * group_width:(group + 1) * group_width]
            partial_value = jnp.dot(columns, out_weight[group * group_width:(group + 1) * group_width], preferred_element_type=jnp.float32)
            partial_value = lax.optimization_barrier(partial_value.astype(jnp.bfloat16))
            branch = branch + partial_value.astype(jnp.float32)
        return (owner_rows.astype(jnp.float32) + branch).astype(jnp.bfloat16)
    outputs = lax.map(per_owner, jnp.arange(N_TOK, dtype=jnp.int32))
    return outputs.reshape(N_TOK, N_TOK, SLOT, D).transpose(1, 0, 2, 3).reshape(TOKENS, D)
```

```python
import jax
import jax.numpy as jnp
from jax import lax
from jax.sharding import PartitionSpec as P

HD = 128
USERS_OWN = 8
BLK = 128


def project(features, uvqk_weight):
    mixed_rows = jnp.einsum(
        "td,dkf->tkf", features, uvqk_weight, preferred_element_type=jnp.float32
    )
    return jax.nn.silu(mixed_rows).astype(jnp.bfloat16)


def positions(segments, user_count):
    user_ids = jnp.arange(user_count, dtype=jnp.int32)
    member = (segments[:, None] == user_ids[None, :]).astype(jnp.int32)
    counts = jnp.sum(member, axis=0)
    firsts = jnp.cumsum(counts) - counts
    first_row = jnp.sum(member * firsts[None, :], axis=1)
    return jnp.arange(segments.shape[0], dtype=jnp.int32) - first_row


def attend(uvqk_rows, segments):
    row_count = uvqk_rows.shape[0]
    heads_here = uvqk_rows.shape[2] // HD
    split_rows = uvqk_rows.reshape(row_count, 4, heads_here, HD)
    gate_rows = split_rows[:, 0]
    value_rows = split_rows[:, 1]
    query_rows = split_rows[:, 2]
    key_rows = split_rows[:, 3]
    blocks = positions(segments, USERS_OWN) // BLK
    scores = jnp.einsum(
        "qhe,khe->hqk", query_rows, key_rows, preferred_element_type=jnp.float32
    ) * HD ** (-0.5)
    allowed = (segments[:, None] == segments[None, :]) & (blocks[None, :] <= blocks[:, None])
    weights = jnp.where(allowed[None], jax.nn.silu(scores), 0.0).astype(jnp.bfloat16)
    mixed_rows = jnp.einsum(
        "hqk,khe->qhe", weights, value_rows, preferred_element_type=jnp.float32
    )
    normed = mixed_rows * lax.rsqrt(
        jnp.mean(mixed_rows * mixed_rows, axis=-1, keepdims=True) + 1e-06
    )
    return (
        (normed * gate_rows.astype(jnp.float32))
        .astype(jnp.bfloat16)
        .reshape(row_count, heads_here * HD)
    )


def swap(value, pair_count):
    return lax.ppermute(value, "head", [(h, h ^ 1) for h in range(pair_count)])


def deal(blocks, owners):
    return [
        blocks[k] if k == 0 else lax.ppermute(blocks[k], "tok", [(s, s ^ k) for s in range(owners)])
        for k in range(owners)
    ]


def per_device(events, uvqk_weight, out_weight, segments):
    owners = lax.axis_size("tok")
    me = lax.axis_index("tok")
    side = lax.axis_index("head")
    row_count, dim_model = events.shape
    slot_rows = row_count // owners
    pair_count = lax.axis_size("head")
    half_rows = slot_rows // pair_count
    half_width = dim_model // pair_count
    sliced = events.reshape(owners, pair_count, half_rows, dim_model)
    picks = [
        lax.dynamic_slice(sliced, (me ^ k, side, 0, 0), (1, 1, half_rows, dim_model))[0, 0]
        for k in range(owners)
    ]
    mine = jnp.stack(deal(picks, owners))
    other = swap(mine, pair_count)
    first = jnp.where(side == 0, mine, other)
    second = jnp.where(side == 0, other, mine)
    joined = jnp.stack([first, second], axis=1).reshape(owners, slot_rows, dim_model)
    order = jnp.arange(owners) ^ me
    rows = jnp.take(joined, order, axis=0).reshape(row_count, dim_model)
    attended = attend(project(rows, uvqk_weight), segments[0])
    partial = jnp.dot(attended, out_weight, preferred_element_type=jnp.float32).astype(jnp.bfloat16)
    halves = partial.reshape(row_count, pair_count, half_width)
    keep = lax.dynamic_index_in_dim(halves, side, 1, keepdims=False)
    give = lax.dynamic_index_in_dim(halves, side ^ 1, 1, keepdims=False)
    branch = keep.astype(jnp.float32) + swap(give, pair_count).astype(jnp.float32)
    residual = lax.dynamic_slice_in_dim(rows, side * half_width, half_width, 1)
    final = (residual.astype(jnp.float32) + branch).astype(jnp.bfloat16)
    final = final.reshape(owners, slot_rows, half_width)
    backs = [lax.dynamic_index_in_dim(final, me ^ k, 0, keepdims=False) for k in range(owners)]
    returned = jnp.stack(deal(backs, owners))
    return jnp.take(returned, order, axis=0).reshape(row_count, half_width)


def solution(mesh):
    in_specs = (
        P(("grp", "tok"), None),
        P(None, None, "head"),
        P("head", None),
        P(("grp", "tok"), None),
    )
    out_specs = P(("grp", "tok"), "head")
    return jax.shard_map(
        per_device, mesh=mesh, in_specs=in_specs, out_specs=out_specs, check_vma=False
    )
```

```python
import functools

import jax
import jax.numpy as jnp
from jax import lax
from jax.experimental import pallas as pl
from jax.experimental.pallas import tpu as pltpu
from jax.sharding import PartitionSpec as P

HD = 128
USERS_OWN = 8
BLK = 128
BLK_BITS = 7
IN_VMEM = pl.BlockSpec(memory_space=pltpu.VMEM)
IN_SMEM = pl.BlockSpec(memory_space=pltpu.SMEM)
PARAMS = pltpu.CompilerParams(vmem_limit_bytes=12 << 20)
F32 = jnp.float32
BF16 = jnp.bfloat16


def half_silu(half):
    return half + half * jnp.tanh(half)


def user_of(row, starts, ends):
    begin, end = 0, ends[-1]
    for start in starts:
        begin = jnp.where(row >= start, start, begin)
    for stop in reversed(ends):
        end = jnp.where(row < stop, stop, end)
    return begin, end


def last_key(row, begin, end):
    return jnp.minimum(end, begin + (lax.shift_right_logical(row - begin, BLK_BITS) + 1) * BLK)


def lay_out_kernel(parts, flat):
    for at in range(0, parts.shape[0], BLK):
        flat[at : at + BLK, :] = parts[at : at + BLK].reshape(BLK, flat.shape[1])


def prepare_kernel(me, out_weight, segments, keep, give, bounds, edges):
    cols = keep.shape[1]
    keep[...] = jnp.where(me[1] == 0, out_weight[:, :cols], out_weight[:, cols:])
    give[...] = jnp.where(me[1] == 0, out_weight[:, cols:], out_weight[:, :cols])
    ids = segments[...].astype(F32)
    counts = [jnp.sum((ids <= user).astype(F32)).astype(jnp.int32) for user in range(USERS_OWN)]
    starts, ends = counts[:-1], counts
    rows = lax.broadcasted_iota(jnp.int32, (bounds.shape[0], 1), 0)
    begin, end = user_of(rows, starts, ends)
    bounds[:, 0:1] = begin
    bounds[:, 1:2] = last_key(rows, begin, end)
    for block in range(bounds.shape[0] // BLK):
        first = block * BLK
        edges[2 * block] = user_of(jnp.int32(first), starts, ends)[0]
        last = jnp.int32(first + BLK - 1)
        edges[2 * block + 1] = last_key(last, *user_of(last, starts, ends))


def project(joined, weight, uvqk, step):
    width = uvqk.shape[2]
    for begin in range(0, joined.shape[0], step):
        rows = joined[begin : begin + step, :]
        for part in range(4):
            raw = jnp.dot(rows, weight[:, part * width : (part + 1) * width], preferred_element_type=F32)
            uvqk[part, begin : begin + step, :] = half_silu(0.5 * raw).astype(BF16)


def attend(edges, bounds, queries, keys, sums, q_home, k_home, step):
    rows, width = sums.shape
    for q in range(rows // BLK):
        q_at = q_home * rows + q * BLK
        q_block = q_home * (rows // BLK) + q
        for k in range(rows // step):
            k_at = k_home * rows + k * step

            @pl.when((k_at < edges[2 * q_block + 1]) & (k_at + step > edges[2 * q_block]))
            def _():
                edge = bounds[pl.ds(pl.multiple_of(q_at, BLK), BLK), :] - k_at
                col = lax.broadcasted_iota(jnp.int32, (BLK, step), 1)
                allowed = ((col >= edge[:, 0:1]) & (col < edge[:, 1:2])).astype(F32)
                q_cut, k_cut = slice(q * BLK, (q + 1) * BLK), slice(k * step, (k + 1) * step)
                for h in range(width // HD):
                    cut = slice(h * HD, (h + 1) * HD)
                    scores = lax.dot_general(
                        queries[2, q_cut, cut],
                        keys[3, k_cut, cut],
                        (((1,), (1,)), ((), ())),
                        preferred_element_type=F32,
                    )
                    weights = (half_silu(scores * (0.5 * HD**-0.5)) * allowed).astype(BF16)
                    sums[q_cut, cut] += jnp.dot(weights, keys[1, k_cut, cut], preferred_element_type=F32)


def finish(joined_half, uvqk, sums, weight_keep, weight_give, give, base, step):
    for begin in range(0, sums.shape[0], step):
        cut_rows = slice(begin, begin + step)
        parts = []
        for h in range(sums.shape[1] // HD):
            cut = slice(h * HD, (h + 1) * HD)
            mixed = sums[cut_rows, cut]
            normed = mixed * lax.rsqrt(jnp.mean(mixed * mixed, axis=-1, keepdims=True) + 1e-06)
            parts.append((normed * uvqk[0, cut_rows, cut].astype(F32)).astype(BF16))
        attended = jnp.concatenate(parts, axis=1)
        give[cut_rows, :] = jnp.dot(attended, weight_give[...], preferred_element_type=F32).astype(BF16)
        keep = jnp.dot(attended, weight_keep[...], preferred_element_type=F32).astype(BF16)
        base[cut_rows, :] = joined_half(cut_rows).astype(F32) + keep.astype(F32)


def join(me, slabs, joined, group, slot):
    half = slot // 2
    for k, mine, other in slabs:
        begin = ((me[0] ^ k) % group) * slot
        for piece, side in ((mine, me[1]), (other, 1 - me[1])):
            joined[pl.ds(pl.multiple_of(begin + side * half, half), half), :] = piece[...]


def near_kernel(ks, group, slot, step, me, edges, bounds, weight, own_first, own_second, *refs):
    count = len(ks)
    uvqk, residual, sums, joined = refs[-4:]
    half = slot // 2
    for side, piece in enumerate((own_first, own_second)):
        spot = pl.multiple_of((me[0] % group) * slot + side * half, half)
        joined[pl.ds(spot, half), :] = piece[...]
    join(me, [(k, refs[i], refs[count + i]) for i, k in enumerate(ks)], joined, group, slot)
    sums[...] = jnp.zeros_like(sums)
    half_width = residual.shape[1]
    residual[...] = jnp.where(me[1] == 0, joined[:, :half_width], joined[:, half_width:])
    project(joined, weight, uvqk, step)
    home = me[0] // group
    attend(edges, bounds, uvqk, uvqk, sums, home, home, step)


def far_kernel(ks, group, slot, step, me, edges, bounds, weight, weight_keep, weight_give, near_uvqk, *refs):
    count = len(ks)
    uvqk, give, base, joined, sums = refs[-5:]
    join(me, [(k, refs[i], refs[count + i]) for i, k in enumerate(ks)], joined, group, slot)
    project(joined, weight, uvqk, step)
    sums[...] = jnp.zeros_like(sums)
    near = me[0] // group
    far = 1 - near
    attend(edges, bounds, uvqk, uvqk, sums, far, far, step)
    attend(edges, bounds, uvqk, near_uvqk, sums, far, near, step)
    half_width = base.shape[1]

    def residual(cut_rows):
        return jnp.where(me[1] == 0, joined[cut_rows, :half_width], joined[cut_rows, half_width:])

    finish(residual, uvqk, sums, weight_keep, weight_give, give, base, step)


def near_end_kernel(group, step, me, edges, bounds, weight_keep, weight_give, near_uvqk, far_uvqk, residual, sums_in, give, base, sums):
    sums[...] = sums_in[...]
    near = me[0] // group
    attend(edges, bounds, near_uvqk, far_uvqk, sums, near, 1 - near, step)
    finish(lambda cut: residual[cut, :], near_uvqk, sums, weight_keep, weight_give, give, base, step)


def add_kernel(ks, group, slot, me, base, given, *outs):
    for k, out in zip(ks, outs):
        spot = pl.ds(pl.multiple_of(((me[0] ^ k) % group) * slot, slot), slot)
        out[...] = (base[spot, :] + given[spot, :].astype(F32)).astype(BF16)


def place_kernel(slot, me, *refs):
    pieces, out, sems = refs[:-2], refs[-2], refs[-1]
    copies = []
    for k, piece in enumerate(pieces):
        spot = pl.ds(pl.multiple_of((me[0] ^ k) * slot, slot), slot)
        copies.append(pltpu.make_async_copy(piece, out.at[spot, :], sems.at[k]))
        copies[-1].start()
    for copy in copies:
        copy.wait()


def call(body, out_shape, operands, in_smem=1, in_hbm=0, out_smem=0, scratch=(), vmem=12):
    return pl.pallas_call(
        body,
        out_shape=out_shape,
        in_specs=[IN_SMEM] * in_smem
        + [pl.BlockSpec(memory_space=pltpu.HBM)] * in_hbm
        + [IN_VMEM] * (len(operands) - in_smem - in_hbm),
        out_specs=[IN_VMEM] * (len(out_shape) - out_smem) + [IN_SMEM] * out_smem,
        scratch_shapes=list(scratch),
        compiler_params=pltpu.CompilerParams(vmem_limit_bytes=vmem << 20),
    )(*operands)


def swap(value):
    return lax.ppermute(value, "head", [(0, 1), (1, 0)])


def exchange(block, k, owners):
    return lax.ppermute(block, "tok", [(s, s ^ k) for s in range(owners)])


def whole_step(events, uvqk_weight, out_weight, segments):
    owners = lax.axis_size("tok")
    me = lax.axis_index("tok")
    side = lax.axis_index("head")
    row_count, dim_model = events.shape
    slot = row_count // owners
    half_width = dim_model // lax.axis_size("head")
    width = uvqk_weight.shape[2]
    group = owners // 2
    rows = row_count // 2
    step = 2 * BLK

    half = slot // 2
    near_ks, far_ks = range(1, group), range(group, owners)

    sliced = events.reshape(owners, 2, half, dim_model)

    def send(k):
        block = lax.dynamic_slice(sliced, (me ^ k, side, 0, 0), (1, 1, half, dim_model))[0, 0]
        return exchange(block, k, owners)

    mine = {k: send(k) for k in range(1, owners)}
    own = [lax.dynamic_slice(sliced, (me, h, 0, 0), (1, 1, half, dim_model))[0, 0] for h in range(2)]
    ids = jnp.stack([me, side]).astype(jnp.int32)

    uvqk_shape = jax.ShapeDtypeStruct((4, rows, width), BF16)
    give_shape = jax.ShapeDtypeStruct((rows, half_width), BF16)
    base_shape = jax.ShapeDtypeStruct((rows, half_width), F32)
    sums_shape = jax.ShapeDtypeStruct((rows, width), F32)
    part_shape = jax.ShapeDtypeStruct((width, half_width), BF16)
    joined = pltpu.VMEM((rows, dim_model), BF16)

    weight_keep, weight_give, bounds, edges = call(
        prepare_kernel,
        [
            part_shape,
            part_shape,
            jax.ShapeDtypeStruct((row_count, 2), jnp.int32),
            jax.ShapeDtypeStruct((2 * (row_count // BLK),), jnp.int32),
        ],
        [ids, out_weight, segments],
        out_smem=1,
    )
    (weight,) = call(lay_out_kernel, [jax.ShapeDtypeStruct((dim_model, 4 * width), BF16)], [uvqk_weight], in_smem=0)
    other = {k: swap(mine[k]) for k in mine}
    near_uvqk, near_residual, near_sums = call(
        functools.partial(near_kernel, near_ks, group, slot, step),
        [uvqk_shape, give_shape, sums_shape],
        [ids, edges, bounds, weight, *own, *[mine[k] for k in near_ks], *[other[k] for k in near_ks]],
        in_smem=2,
        scratch=[joined],
    )
    far_uvqk, far_give, far_base = call(
        functools.partial(far_kernel, far_ks, group, slot, step),
        [uvqk_shape, give_shape, base_shape],
        [ids, edges, bounds, weight, weight_keep, weight_give, near_uvqk]
        + [mine[k] for k in far_ks]
        + [other[k] for k in far_ks],
        in_smem=2,
        scratch=[joined, pltpu.VMEM((rows, width), F32)],
    )
    far_given = swap(far_give)
    near_give, near_base = call(
        functools.partial(near_end_kernel, group, step),
        [give_shape, base_shape],
        [ids, edges, bounds, weight_keep, weight_give, near_uvqk, far_uvqk, near_residual, near_sums],
        in_smem=2,
        scratch=[pltpu.VMEM((rows, width), F32)],
    )
    near_given = swap(near_give)
    returned = [None] * owners
    for ks, base, given in ((range(group, owners), far_base, far_given), (range(group), near_base, near_given)):
        finals = call(
            functools.partial(add_kernel, ks, group, slot),
            [jax.ShapeDtypeStruct((slot, half_width), BF16)] * group,
            [ids, base, given],
        )
        for k, final in zip(ks, finals):
            returned[k] = final if k == 0 else exchange(final, k, owners)
    return pl.pallas_call(
        functools.partial(place_kernel, slot),
        out_shape=jax.ShapeDtypeStruct((row_count, half_width), BF16),
        in_specs=[IN_SMEM] + [pl.BlockSpec(memory_space=pl.ANY)] * owners,
        out_specs=pl.BlockSpec(memory_space=pl.ANY),
        scratch_shapes=[pltpu.SemaphoreType.DMA((owners,))],
        compiler_params=PARAMS,
        name="place",
    )(ids, *returned)


def solution(mesh):
    in_specs = (
        P(("grp", "tok"), None),
        P(None, None, "head"),
        P("head", None),
        P(("grp", "tok"), None),
    )
    out_specs = P(("grp", "tok"), "head")
    return jax.shard_map(whole_step, mesh=mesh, in_specs=in_specs, out_specs=out_specs, check_vma=False)
```
